32 devices in a mesh: pages: 8 (over y, x, core), heads: 4 (over z).
Axes of the slice: x: 2, y: 2, z: 4, core: 2. Of those that a mesh axis runs over, the one named last changes fastest.
Arguments:
- queries: bfloat16 [512, 32, 128], P('pages', 'heads'), may hold values from -6 to 6
- keys: bfloat16 [576, 16, 128, 128], P('pages', 'heads'), may hold values from -6 to 6
- values: bfloat16 [576, 16, 128, 128], P('pages', 'heads'), may hold values from -6 to 6
- hot_pages: int32 [64], replicated, may hold values from 0 to 575, as said below
- hot_used: int32 [512], replicated, may hold values from 1 to 64
- user_pages: int32 [512, 1], P('pages'), may hold values from 8 to 71, as said below
- lengths: int32 [512], P('pages'), may hold values from 1 to 128
- o_weight: bfloat16 [4096, 4608], P('heads'), may hold values from -0.09375 to 0.09375
- residual: bfloat16 [512, 4608], P(('pages', 'heads')), may hold values from -6 to 6
- norm_gain: float32 [4608], replicated, may hold values from 0.25 to 1.75
Outputs:
- output: bfloat16 [512, 4608], P(('pages', 'heads'))
The draws below stay inside these ranges and needn't reach their ends.
Inputs may be any that keep to these rules, and one draw needn't show every extreme that they name: `hot_pages`: 64 distinct pages; each lies among the first 8 pages of its group (page p belongs to group p // 72); one group holds exactly 8 of them and none holds more. `user_pages`: numbers within the sequence's own group (sequence s belongs to group s // 64); all own pages of the sequences of one group are distinct.
All inputs are finite; a program needn't handle non-finite values.
Results may differ from the reference program's by a relative error of at most 0.019.
Values may be sent and summed in bfloat16 or wider, within the bound.
No kernel may reach another device: no remote copies, remote signals or barrier semaphores. Data moves between devices by JAX's collectives and lax.ppermute only.
A program may use at most 128 MiB of HBM per device.

```python
import jax
import jax.numpy as jnp
from jax import lax

DM = 4608
QH = 32
KVH = 16
HD = 128
PAGE = 128
HOT = 64
HOT_CAP = 8
UPS = 1
SEQ_DEV = 64
PG_DEV = 72
GROUPS = 8
PAGES = 576
SEQS = 512


def draw_hot_pages(key, part):
    key_full, key_rank, key_order = jax.random.split(jax.random.fold_in(key, 11), 3)
    slot_ids = jnp.arange(GROUPS * HOT_CAP, dtype=jnp.int32)
    group_of = slot_ids // HOT_CAP
    within = slot_ids % HOT_CAP
    full_group = jax.random.randint(key_full, (), 0, GROUPS, dtype=jnp.int32)
    ranking = jax.random.permutation(key_rank, GROUPS * HOT_CAP).astype(jnp.int32)
    priority = jnp.where(group_of == full_group, within - HOT_CAP, ranking)
    chosen = jnp.argsort(priority, stable=True)[:HOT]
    picked = (group_of * PG_DEV + within)[chosen]
    return jax.random.permutation(key_order, picked).astype(jnp.int32)


def draw_user_pages(key, part):
    group_keys = jax.random.split(jax.random.fold_in(key, 23), GROUPS)

    def one_group(group_key):
        return jax.random.permutation(group_key, PG_DEV - HOT_CAP)[:SEQ_DEV * UPS].astype(jnp.int32)
    picked = jax.vmap(one_group)(group_keys) + HOT_CAP
    return picked.reshape(SEQS, UPS).astype(jnp.int32)


def place_ends(entries, key, smallest, high):
    longest = entries.shape.index(max(entries.shape))
    spots = []
    for shift in (0, 1):
        where = [jax.random.randint(jax.random.fold_in(key, axis), (), 0, length) for axis, length in enumerate(entries.shape)]
        where[longest] = (where[longest] + shift) % entries.shape[longest]
        spots.append(tuple(where))
    return entries.at[spots[0]].set(smallest).at[spots[1]].set(high)


def block_levels(own_key, dims, shards, least, top_value):
    loudness = 1.0
    for position, shards_of in shards:
        draws = jax.random.uniform(jax.random.fold_in(jax.random.fold_in(own_key, 6), position), (shards_of,), jnp.float32, least / len(shards), top_value / len(shards))
        loudness = loudness * jnp.repeat(jnp.exp(draws), dims[position] // shards_of).reshape((-1,) + (1,) * (len(dims) - 1 - position))
    return loudness


def normal_values(stream_key, shape, spread, most, shards=(), kind=jnp.bfloat16):
    array = jax.random.normal(stream_key, shape, jnp.float32) * spread
    if len(shards) > 0:
        array = block_levels(stream_key, shape, shards, -0.22, 0.18) * array
    return jnp.clip(array, min=-most, max=most).astype(kind)


def setup_inputs(seed: int = 0) -> dict:
    arg_keys = jax.random.split(jax.random.key(seed), 11)
    return {
        "queries": normal_values(arg_keys[0], (SEQS, QH, HD), 1.0, 6.0, ((0, 8), (1, 4))),
        "keys": normal_values(arg_keys[1], (PAGES, KVH, PAGE, HD), 1.0, 6.0, ((0, 8), (1, 4))),
        "values": normal_values(arg_keys[2], (PAGES, KVH, PAGE, HD), 1.0, 6.0, ((0, 8), (1, 4))),
        "hot_pages": draw_hot_pages(jax.random.fold_in(arg_keys[10], 71), 0),
        "hot_used": place_ends(jax.random.randint(arg_keys[4], (SEQS,), 1, HOT + 1), jax.random.fold_in(arg_keys[4], 1), 1, HOT).astype(jnp.int32),
        "user_pages": draw_user_pages(jax.random.fold_in(arg_keys[10], 71), 0),
        "lengths": place_ends(jax.random.randint(arg_keys[6], (SEQS,), 1, UPS * PAGE + 1), jax.random.fold_in(arg_keys[6], 1), 1, UPS * PAGE).astype(jnp.int32),
        "o_weight": normal_values(arg_keys[7], (QH * HD, DM), (QH * HD) ** -0.5, 0.09375, ((0, 4),)),
        "residual": normal_values(arg_keys[8], (SEQS, DM), 1.0, 6.0, ((0, 32),)),
        "norm_gain": jnp.clip(1.0 + 0.15 * jax.random.normal(arg_keys[9], (DM,), jnp.float32), 0.25, 1.75),
    }


score_scale = 1.0 / 12.0
soft_cap = 50.0
epsilon = 1e-06

def reference(queries, keys, values, hot_pages, hot_used, user_pages, lengths, o_weight, residual, norm_gain):
    group_size = QH // KVH
    seq_total = queries.shape[0]
    owner_base = jnp.arange(seq_total, dtype=jnp.int32) // SEQ_DEV * PG_DEV
    user_ids = (owner_base[:, None] + user_pages).astype(jnp.int32)
    hot_token_page = jnp.arange(HOT * PAGE, dtype=jnp.int32) // PAGE
    hot_mask = hot_token_page[None, :] < hot_used[:, None]
    user_mask = jnp.arange(UPS * PAGE, dtype=jnp.int32)[None, :] < lengths[:, None]

    def weights_of(logits, allowed):
        weight = jnp.exp(soft_cap * jnp.tanh(logits * score_scale / soft_cap))
        weight = jnp.where(allowed, weight, jnp.float32(0.0))
        rounded = lax.optimization_barrier(weight.astype(jnp.bfloat16))
        return (weight, rounded.astype(jnp.float32))

    def per_head(kv_index):
        query_f32 = lax.dynamic_slice_in_dim(queries, kv_index * group_size, group_size, 1).astype(jnp.float32)
        hot_keys = keys[hot_pages, kv_index].reshape(HOT * PAGE, HD).astype(jnp.float32)
        hot_values = values[hot_pages, kv_index].reshape(HOT * PAGE, HD).astype(jnp.float32)
        own_keys = keys[user_ids, kv_index].reshape(seq_total, UPS * PAGE, HD).astype(jnp.float32)
        own_values = values[user_ids, kv_index].reshape(seq_total, UPS * PAGE, HD).astype(jnp.float32)
        hot_logits = jnp.einsum('sgd,td->sgt', query_f32, hot_keys)
        hot_weight, hot_rounded = weights_of(hot_logits, hot_mask[:, None, :])
        own_logits = jnp.einsum('sgd,std->sgt', query_f32, own_keys)
        own_weight, own_rounded = weights_of(own_logits, user_mask[:, None, :])
        numerator = jnp.einsum('sgt,td->sgd', hot_rounded, hot_values) + jnp.einsum('sgt,std->sgd', own_rounded, own_values)
        totals = lax.optimization_barrier(jnp.sum(hot_weight, axis=2)) + lax.optimization_barrier(jnp.sum(own_weight, axis=2))
        return (numerator / totals[:, :, None]).astype(jnp.bfloat16)
    per_kv = lax.map(per_head, jnp.arange(KVH, dtype=jnp.int32))
    attended = jnp.transpose(per_kv, (1, 0, 2, 3)).reshape(seq_total, QH * HD)
    projected = jnp.dot(attended, o_weight, preferred_element_type=jnp.float32)
    mean_sq = lax.optimization_barrier(jnp.mean(projected * projected, axis=1, keepdims=True))
    normed = projected / jnp.sqrt(mean_sq + epsilon) * norm_gain[None, :]
    return (residual.astype(jnp.float32) + normed).astype(jnp.bfloat16)
```

```python
import functools
import math

import jax
import jax.numpy as jnp
from jax import lax
from jax.experimental import pallas as pl
from jax.experimental.pallas import tpu as pltpu
from jax.sharding import PartitionSpec as P

HOT_CAP = 8
score_scale = 1.0 / 12.0
soft_cap = 50.0
epsilon = 1e-06
inner = score_scale / soft_cap
outer = soft_cap * math.log2(math.e)
MIB = 1 << 20


def weights_of(logits):
    return jnp.exp2(outer * jnp.tanh(logits * inner))


def dot_t(a, b):
    return lax.dot_general(a, b, (((1,), (1,)), ((), ())), preferred_element_type=jnp.float32)


def dot_n(a, b):
    return lax.dot_general(a, b, (((1,), (0,)), ((), ())), preferred_element_type=jnp.float32)


def own_kernel(
    seqs, ups, heads, group, kv_heads, unroll,
    pages_ref, lengths_ref, q_ref, keys_ref, values_ref, num_ref, tot_ref, kbuf, vbuf, ksem, vsem,
):
    page_len, head_dim = kbuf.shape[2], kbuf.shape[3]
    width = kv_heads * page_len

    def copies(i):
        page = pages_ref[i]
        return (
            pltpu.make_async_copy(keys_ref.at[page], kbuf.at[i], ksem.at[i]),
            pltpu.make_async_copy(values_ref.at[page], vbuf.at[i], vsem.at[i]),
        )

    def start(i, carry):
        for copy in copies(i):
            copy.start()
        return carry

    lax.fori_loop(0, seqs * ups, start, 0)
    column = lax.broadcasted_iota(jnp.int32, (heads, width), 1)
    row = lax.broadcasted_iota(jnp.int32, (heads, width), 0)
    mine = (column // page_len) == (row // group)
    token = column % page_len
    ones = jnp.ones((width, head_dim), jnp.bfloat16)

    def block(b, carry):
        for j in range(unroll):
            for u in range(ups):
                for copy in copies((b * unroll + j) * ups + u):
                    copy.wait()
        for j in range(unroll):
            s = b * unroll + j
            q = q_ref[pl.ds(pl.multiple_of(s * heads, heads), heads), :]
            total = jnp.zeros((heads, 2 * head_dim), jnp.float32)
            for u in range(ups):
                k = kbuf[s * ups + u].reshape(width, head_dim)
                v = vbuf[s * ups + u].reshape(width, head_dim)
                allowed = mine & (token + u * page_len < lengths_ref[s])
                weight = jnp.where(allowed, weights_of(dot_t(q, k)), 0.0).astype(jnp.bfloat16)
                total = total + dot_n(weight, jnp.concatenate([v, ones], axis=1))
            num_ref[pl.ds(s, heads, stride=seqs), :] = total[:, :head_dim]
            tot_ref[pl.ds(s, heads, stride=seqs), :] = total[:, head_dim:]
        return carry

    lax.fori_loop(0, seqs // unroll, block, 0)


def own_terms(q, keys, values, user_pages, lengths):
    seqs, ups = user_pages.shape
    _, kv_heads, page_len, head_dim = keys.shape
    group = q.shape[1] // kv_heads
    heads = -(-q.shape[1] // 8) * 8
    q = jnp.pad(q, ((0, 0), (0, heads - q.shape[1]), (0, 0))).reshape(seqs * heads, head_dim)
    unroll = math.gcd(seqs, 16)
    any_space = pl.BlockSpec(memory_space=pltpu.HBM)
    whole = pl.BlockSpec(memory_space=pltpu.VMEM)
    out = jax.ShapeDtypeStruct((heads * seqs, head_dim), jnp.float32)
    count = seqs * ups
    buf = pltpu.VMEM((count, kv_heads, page_len, head_dim), jnp.bfloat16)
    return pl.pallas_call(
        functools.partial(own_kernel, seqs, ups, heads, group, kv_heads, unroll),
        out_shape=(out, out),
        in_specs=[pl.BlockSpec(memory_space=pltpu.SMEM)] * 2 + [whole, any_space, any_space],
        out_specs=(whole, whole),
        scratch_shapes=[buf, buf, pltpu.SemaphoreType.DMA((count,)), pltpu.SemaphoreType.DMA((count,))],
        compiler_params=pltpu.CompilerParams(vmem_limit_bytes=24 * MIB),
        name="own_pages",
    )(
        user_pages.reshape(count),
        lengths,
        q,
        pltpu.with_memory_space_constraint(keys, pltpu.HBM),
        pltpu.with_memory_space_constraint(values, pltpu.HBM),
    )


def hot_kernel(sources, seqs, heads, kv_heads, packed, pos_ref, *refs):
    used = refs[:sources]
    queries = refs[sources : 2 * sources]
    halves = (refs[2 * sources : 2 * sources + 2], refs[2 * sources + 2 : 2 * sources + 4])
    outs = refs[2 * sources + 4 : -2]
    staged, totals = refs[-2:]
    group = heads // kv_heads
    h = pl.program_id(0)
    cap, _, page_len, head_dim = halves[0][0].shape
    lane = lax.broadcasted_iota(jnp.int32, (seqs, head_dim), 1)

    @pl.when(h == 0)
    def _():
        for r in range(sources):
            staged[r] = queries[r][...].astype(jnp.float32)
        totals[...] = jnp.zeros_like(totals)

    rows = [
        staged[r, pl.ds(h * group + g, seqs, stride=heads), :].astype(jnp.bfloat16)
        for r in range(sources)
        for g in range(group)
    ]
    q = jnp.concatenate(rows, axis=0)
    used_rows = [u[...] for u in used]
    step = math.gcd(cap, 4)
    ones = jnp.ones((step * page_len, head_dim), jnp.bfloat16)
    acc = jnp.zeros((q.shape[0], 2 * head_dim), jnp.float32)
    for half, (k_ref, v_ref) in enumerate(halves):
        for c in range(0, cap, step):
            k = k_ref[c : c + step].reshape(step * page_len, head_dim)
            v = v_ref[c : c + step].reshape(step * page_len, head_dim)
            weight = weights_of(dot_t(q, k))
            parts = []
            for p in range(step):
                place = pos_ref[half * cap + c + p]
                masks = [u > place for u in used_rows for _ in range(group)]
                part = [
                    jnp.where(m, weight[i * seqs : (i + 1) * seqs, p * page_len : (p + 1) * page_len], 0.0)
                    for i, m in enumerate(masks)
                ]
                parts.append(jnp.concatenate(part, axis=0).astype(jnp.bfloat16))
            acc = acc + dot_n(jnp.concatenate(parts, axis=1), jnp.concatenate([v, ones], axis=1))
    for r in range(sources):
        for g in range(group):
            i = r * group + g
            head = h * group + g
            num = acc[i * seqs : (i + 1) * seqs, :head_dim]
            tot = acc[i * seqs : (i + 1) * seqs, head_dim:]
            if packed:
                rest = tot - tot.astype(jnp.bfloat16).astype(jnp.float32)
                outs[r][head] = num.astype(jnp.bfloat16)
                totals[r] = jnp.where(lane == head, tot, jnp.where(lane == heads + head, rest, totals[r]))
            else:
                outs[2 * r][pl.ds(pl.multiple_of(head * seqs, seqs), seqs), :] = num
                outs[2 * r + 1][pl.ds(pl.multiple_of(head * seqs, seqs), seqs), :] = tot
    if packed:

        @pl.when(h == kv_heads - 1)
        def _():
            for r in range(sources):
                outs[r][heads] = totals[r].astype(jnp.bfloat16)


def hot_terms(queries, used, position, own_kv, partner_kv, packed):
    sources = len(queries)
    seqs = used[0].shape[0]
    _, kv_heads, page_len, head_dim = own_kv[0].shape
    heads = queries[0].shape[0] // seqs
    kv_spec = pl.BlockSpec((HOT_CAP, 1, page_len, head_dim), lambda h, *_: (0, h, 0, 0))

    def fixed(shape):
        return pl.BlockSpec(shape, lambda h, *_: (0,) * len(shape))

    if packed:
        shapes = [((heads + 1, seqs, head_dim), jnp.bfloat16)] * sources
    else:
        shapes = [((heads * seqs, head_dim), jnp.float32)] * (2 * sources)
    return pl.pallas_call(
        functools.partial(hot_kernel, sources, seqs, heads, kv_heads, packed),
        out_shape=[jax.ShapeDtypeStruct(*s) for s in shapes],
        grid_spec=pltpu.PrefetchScalarGridSpec(
            num_scalar_prefetch=1,
            grid=(kv_heads,),
            in_specs=[fixed(u.shape) for u in used]
            + [fixed(q.shape) for q in queries]
            + [kv_spec] * 4,
            out_specs=[fixed(s[0]) for s in shapes],
            scratch_shapes=[
                pltpu.VMEM((sources, seqs * heads, head_dim), jnp.float32),
                pltpu.VMEM((sources, seqs, head_dim), jnp.float32),
            ],
        ),
        compiler_params=pltpu.CompilerParams(
            dimension_semantics=("arbitrary",), vmem_limit_bytes=20 * MIB
        ),
        name="hot_pages",
    )(position, *used, *queries, *own_kv, *partner_kv)


def project_kernel(received, seqs, heads, ways, z_ref, *refs):
    blocks = refs[:received]
    own_num, own_tot, hot_num, hot_tot, w_ref = refs[received : received + 5]
    outs = refs[received + 5 : received + 5 + ways]
    spread, att = refs[-2:]
    head_dim = own_num.shape[1]
    rows = seqs // ways

    @pl.when(pl.program_id(0) == 0)
    def _():
        far = jnp.zeros((seqs, head_dim), jnp.float32)
        for b in blocks:
            far = far + b[heads].astype(jnp.float32)
        for h in range(heads):
            part = pl.ds(h * seqs, seqs)
            num = own_num[part, :] + hot_num[part, :]
            tot = own_tot[part, :] + hot_tot[part, :]
            for b in blocks:
                num = num + b[h].astype(jnp.float32)
            if blocks:
                tot = tot + (far[:, h : h + 1] + far[:, heads + h : heads + h + 1])
            spread[:, h * head_dim : (h + 1) * head_dim] = num / tot
        for k in range(ways):
            target = lax.rem(z_ref[0] + k, ways)
            att[k * rows : (k + 1) * rows, :] = spread[
                pl.ds(pl.multiple_of(target * rows, rows), rows), :
            ].astype(jnp.bfloat16).astype(jnp.float32)

    res = dot_n(att[...].astype(jnp.bfloat16), w_ref[...])
    for k in range(ways):
        outs[k][...] = res[k * rows : (k + 1) * rows].astype(outs[k].dtype)


def project(blocks, own, hot, o_weight, z, ways):
    head_dim = own[0].shape[1]
    width, model = o_weight.shape
    heads = width // head_dim
    seqs = hot[0].shape[0] // heads
    rows = seqs // ways
    tile = math.gcd(model, 768)

    def fixed(x):
        return pl.BlockSpec(x.shape, lambda n, *_: (0,) * x.ndim)

    kinds = [jnp.float32] + [jnp.bfloat16] * (ways - 1)
    return pl.pallas_call(
        functools.partial(project_kernel, len(blocks), seqs, heads, ways),
        out_shape=[jax.ShapeDtypeStruct((rows, model), kind) for kind in kinds],
        grid_spec=pltpu.PrefetchScalarGridSpec(
            num_scalar_prefetch=1,
            grid=(model // tile,),
            in_specs=[fixed(b) for b in blocks]
            + [fixed(x) for x in (*own, *hot)]
            + [pl.BlockSpec((width, tile), lambda n, *_: (0, n))],
            out_specs=[pl.BlockSpec((rows, tile), lambda n, *_: (0, n))] * ways,
            scratch_shapes=[
                pltpu.VMEM((seqs, width), jnp.float32),
                pltpu.VMEM((seqs, width), jnp.float32),
            ],
        ),
        compiler_params=pltpu.CompilerParams(
            dimension_semantics=("arbitrary",), vmem_limit_bytes=20 * MIB
        ),
        name="project",
    )(z, *blocks, *own, *hot, o_weight)


def norm_kernel(*refs):
    parts, (residual, gain, out) = refs[:-3], refs[-3:]
    projected = parts[0][...]
    for p in parts[1:]:
        projected = projected + p[...].astype(jnp.float32)
    mean_sq = jnp.mean(projected * projected, axis=1, keepdims=True)
    normed = projected / jnp.sqrt(mean_sq + epsilon) * gain[...]
    out[...] = (residual[...].astype(jnp.float32) + normed).astype(jnp.bfloat16)


def finish(parts, residual, norm_gain):
    return pl.pallas_call(
        norm_kernel,
        out_shape=jax.ShapeDtypeStruct(residual.shape, residual.dtype),
        compiler_params=pltpu.CompilerParams(vmem_limit_bytes=8 * MIB),
        name="finish",
    )(*parts, residual, norm_gain.reshape(1, -1))


def per_device(
    chips, ways, queries, keys, values, hot_pages, hot_used, user_pages, lengths, o_weight, residual, norm_gain
):
    seqs, heads, head_dim = queries.shape
    page_count = keys.shape[0]
    me = lax.axis_index("pages")
    z = lax.axis_index("heads")
    devices = 2 * chips
    swap = [(i, i ^ 1) for i in range(devices)]
    power = chips & (chips - 1) == 0

    def there(i, k):
        return i ^ (2 * k) if power else (i + 2 * k) % devices

    q = queries.reshape(seqs * heads, head_dim)
    out_perm = [[(i, there(i, k)) for i in range(devices)] for k in range(chips)]
    back_perm = [[(j, i) for i, j in perm] for perm in out_perm]
    far_q = [lax.ppermute(q, "pages", out_perm[k]) for k in range(1, chips)]
    own_kv = (keys[:HOT_CAP], values[:HOT_CAP])
    partner_kv = tuple(lax.ppermute(x, "pages", swap) for x in own_kv)

    slot = jnp.arange(2 * HOT_CAP, dtype=jnp.int32)
    holder = jnp.where(slot < HOT_CAP, me, me ^ 1)
    page_ids = holder * page_count + slot % HOT_CAP
    matches = page_ids[:, None] == hot_pages[None, :]
    order = jnp.arange(hot_pages.shape[0], dtype=jnp.int32)
    absent = jnp.int32(jnp.iinfo(jnp.int32).max)
    position = jnp.min(jnp.where(matches, order[None, :], absent), axis=1)
    used_all = hot_used.reshape(devices, seqs)

    def used_of(k):
        origin = me ^ (2 * k) if power else lax.rem(me + devices - 2 * k, devices)
        row = lax.dynamic_index_in_dim(used_all, origin, 0, keepdims=False)
        return jnp.broadcast_to(row[:, None], (seqs, head_dim))

    own = own_terms(queries, keys, values, user_pages, lengths)
    blocks = []
    if chips > 1:
        own, far_q = lax.optimization_barrier((own, far_q))
        sent = hot_terms(
            far_q, [used_of(k) for k in range(1, chips)], position, own_kv, partner_kv, True
        )
        blocks = [lax.ppermute(sent[k - 1], "pages", back_perm[k]) for k in range(1, chips)]
        q, sent = lax.optimization_barrier((q, sent))
    hot = hot_terms([q], [used_of(0)], position, own_kv, partner_kv, False)
    parts = project(blocks, own, hot, o_weight, z.reshape(1), ways)
    arrived = [parts[0]] + [
        lax.ppermute(parts[k], "heads", [(i, (i + k) % ways) for i in range(ways)])
        for k in range(1, ways)
    ]
    return finish(arrived, residual, norm_gain)


def solution(mesh):
    in_specs = (
        P("pages", "heads", None),
        P("pages", "heads", None, None),
        P("pages", "heads", None, None),
        P(),
        P(),
        P("pages", None),
        P("pages"),
        P("heads", None),
        P(("pages", "heads"), None),
        P(),
    )
    out_specs = P(("pages", "heads"), None)
    body = functools.partial(per_device, mesh.shape["pages"] // 2, mesh.shape["heads"])
    return jax.shard_map(body, mesh=mesh, in_specs=in_specs, out_specs=out_specs, check_vma=False)
```

```python
import functools
import math

import jax
import jax.numpy as jnp
from jax import lax
from jax.experimental import pallas as pl
from jax.experimental.pallas import tpu as pltpu
from jax.sharding import PartitionSpec as P


HOT_CAP = 8
score_scale = 1.0 / 12.0
soft_cap = 50.0
epsilon = 1e-06
inner = score_scale / soft_cap
outer = soft_cap * math.log2(math.e)
MIB = 1 << 20


def weights_of(logits):
    return jnp.exp2(outer * jnp.tanh(logits * inner))


def dot_t(a, b):
    return lax.dot_general(a, b, (((1,), (1,)), ((), ())), preferred_element_type=jnp.float32)


def dot_n(a, b):
    return lax.dot_general(a, b, (((1,), (0,)), ((), ())), preferred_element_type=jnp.float32)


def lead_kernel(keys_ref, values_ref, k_out, v_out, sems):
    copies = [
        pltpu.make_async_copy(src.at[pl.ds(0, dst.shape[0])], dst, sems.at[i])
        for i, (src, dst) in enumerate(((keys_ref, k_out), (values_ref, v_out)))
    ]
    for copy in copies:
        copy.start()
    for copy in copies:
        copy.wait()


def in_hbm(x):
    return pltpu.with_memory_space_constraint(x, pltpu.HBM)


HBM = pl.BlockSpec(memory_space=pltpu.HBM)
VMEM = pl.BlockSpec(memory_space=pltpu.VMEM)
SMEM = pl.BlockSpec(memory_space=pltpu.SMEM)


def lead_pages(keys, values):
    out = jax.ShapeDtypeStruct((HOT_CAP, *keys.shape[1:]), keys.dtype)
    return pl.pallas_call(
        lead_kernel,
        out_shape=(out, out),
        in_specs=[HBM, HBM],
        out_specs=(VMEM, VMEM),
        scratch_shapes=[pltpu.SemaphoreType.DMA((2,))],
        compiler_params=pltpu.CompilerParams(vmem_limit_bytes=4 * MIB),
        name="lead_pages",
    )(in_hbm(keys), in_hbm(values))


def own_kernel(
    seqs, ups, heads, group, kv_heads, unroll,
    lengths_ref, q_ref, kbuf, vbuf, w_hbm, num_ref, tot_ref, w_ref, sem,
):
    page_len, head_dim = kbuf.shape[2], kbuf.shape[3]
    width = kv_heads * page_len
    prefetch = pltpu.make_async_copy(w_hbm, w_ref, sem)
    prefetch.start()
    column = lax.broadcasted_iota(jnp.int32, (heads, width), 1)
    row = lax.broadcasted_iota(jnp.int32, (heads, width), 0)
    mine = (column // page_len) == (row // group)
    token = jnp.where(mine, column % page_len, ups * page_len)
    ones = jnp.ones((width, head_dim), jnp.bfloat16)

    def block(b, carry):
        for j in range(unroll):
            s = b * unroll + j
            q = q_ref[pl.ds(pl.multiple_of(s * heads, heads), heads), :]
            total = jnp.zeros((heads, 2 * head_dim), jnp.float32)
            for u in range(ups):
                k = kbuf[s * ups + u].reshape(width, head_dim)
                v = vbuf[s * ups + u].reshape(width, head_dim)
                allowed = token < lengths_ref[s] - u * page_len
                weight = jnp.where(allowed, weights_of(dot_t(q, k)), 0.0).astype(jnp.bfloat16)
                total = total + dot_n(weight, jnp.concatenate([v, ones], axis=1))
            num_ref[pl.ds(s, heads, stride=seqs), :] = total[:, :head_dim]
            tot_ref[pl.ds(s, heads, stride=seqs), :] = total[:, head_dim:]
        return carry

    lax.fori_loop(0, seqs // unroll, block, 0)
    prefetch.wait()


def own_terms(q, own_k, own_v, lengths, o_weight):
    seqs, _, head_dim = q.shape
    count, kv_heads, _, _ = own_k.shape
    group = q.shape[1] // kv_heads
    heads = -(-q.shape[1] // 8) * 8
    q = jnp.pad(q, ((0, 0), (0, heads - q.shape[1]), (0, 0))).reshape(seqs * heads, head_dim)
    unroll = math.gcd(seqs, 32)
    out = jax.ShapeDtypeStruct((heads * seqs, head_dim), jnp.float32)
    num, tot, w = pl.pallas_call(
        functools.partial(own_kernel, seqs, count // seqs, heads, group, kv_heads, unroll),
        out_shape=(out, out, jax.ShapeDtypeStruct(o_weight.shape, o_weight.dtype)),
        in_specs=[SMEM, VMEM, VMEM, VMEM, HBM],
        out_specs=(VMEM, VMEM, VMEM),
        scratch_shapes=[pltpu.SemaphoreType.DMA],
        compiler_params=pltpu.CompilerParams(vmem_limit_bytes=8 * MIB),
        name="own_pages",
    )(lengths, q, own_k, own_v, in_hbm(o_weight))
    return (num, tot), w


def hot_kernel(sources, seqs, heads, kv_heads, packed, fetch, pos_ref, *refs):
    if fetch:
        pages_ref, cache_ref, *refs = refs
        *refs, pages_out, staged, sems = refs

        def copy(i):
            return pltpu.make_async_copy(cache_ref.at[pages_ref[i]], pages_out.at[i], sems.at[i])

        def start(i, carry):
            copy(i).start()
            return carry

        def wait(i, carry):
            copy(i).wait()
            return carry

        lax.fori_loop(0, fetch, start, 0)
    else:
        *refs, staged = refs
    used = refs[:sources]
    queries = refs[sources : 2 * sources]
    halves = (refs[2 * sources : 2 * sources + 2], refs[2 * sources + 2 : 2 * sources + 4])
    outs = refs[2 * sources + 4 :]
    group = heads // kv_heads
    cap, _, page_len, head_dim = halves[0][0].shape
    lane = lax.broadcasted_iota(jnp.int32, (seqs, head_dim), 1)
    for r in range(sources):
        staged[r] = queries[r][...].astype(jnp.float32)
    used_rows = [u[...] for u in used]
    step = 2
    ones = jnp.ones((step * page_len, head_dim), jnp.bfloat16)
    totals = [jnp.zeros((seqs, head_dim), jnp.float32) for _ in range(sources)]
    for h in range(kv_heads):
        rows = [
            staged[r, pl.ds(h * group + g, seqs, stride=heads), :].astype(jnp.bfloat16)
            for r in range(sources)
            for g in range(group)
        ]
        q = jnp.concatenate(rows, axis=0)
        acc = jnp.zeros((q.shape[0], 2 * head_dim), jnp.float32)
        for half, (k_ref, v_ref) in enumerate(halves):
            for c in range(0, cap, step):
                k = k_ref[c : c + step, h].reshape(step * page_len, head_dim)
                v = v_ref[c : c + step, h].reshape(step * page_len, head_dim)
                weight = weights_of(dot_t(q, k))
                parts = []
                for p in range(step):
                    place = pos_ref[half * cap + c + p]
                    columns = slice(p * page_len, (p + 1) * page_len)
                    part = []
                    for r in range(sources):
                        mask = used_rows[r] > place
                        for i in range(r * group, (r + 1) * group):
                            part.append(jnp.where(mask, weight[i * seqs : (i + 1) * seqs, columns], 0.0))
                    parts.append(jnp.concatenate(part, axis=0).astype(jnp.bfloat16))
                acc = acc + dot_n(jnp.concatenate(parts, axis=1), jnp.concatenate([v, ones], axis=1))
        for r in range(sources):
            for g in range(group):
                i = r * group + g
                head = h * group + g
                num = acc[i * seqs : (i + 1) * seqs, :head_dim]
                tot = acc[i * seqs : (i + 1) * seqs, head_dim:]
                if packed:
                    rest = tot - tot.astype(jnp.bfloat16).astype(jnp.float32)
                    outs[r][head] = num.astype(jnp.bfloat16)
                    low = jnp.where(lane == heads + head, rest, totals[r])
                    totals[r] = jnp.where(lane == head, tot, low)
                else:
                    outs[2 * r][head * seqs : (head + 1) * seqs, :] = num
                    outs[2 * r + 1][head * seqs : (head + 1) * seqs, :] = tot
    if packed:
        for r in range(sources):
            outs[r][heads] = totals[r].astype(jnp.bfloat16)
    if fetch:
        lax.fori_loop(0, fetch, wait, 0)


def hot_terms(queries, used, position, own_kv, partner_kv, packed, pages=None, cache=None):
    sources = len(queries)
    seqs = used[0].shape[0]
    _, kv_heads, page_len, head_dim = own_kv[0].shape
    heads = queries[0].shape[0] // seqs
    if packed:
        shapes = [((heads + 1, seqs, head_dim), jnp.bfloat16)] * sources
    else:
        shapes = [((heads * seqs, head_dim), jnp.float32)] * (2 * sources)
    scratch = [pltpu.VMEM((sources, seqs * heads, head_dim), jnp.float32)]
    operands = [position, *used, *queries, *own_kv, *partner_kv]
    specs = [SMEM] + [VMEM] * (2 * sources + 4)
    count = 0
    if pages is not None:
        count = pages.shape[0]
        operands[1:1] = [pages, in_hbm(cache)]
        specs[1:1] = [SMEM, HBM]
        shapes.append(((count, kv_heads, page_len, head_dim), cache.dtype))
        scratch.append(pltpu.SemaphoreType.DMA((count,)))
    return pl.pallas_call(
        functools.partial(hot_kernel, sources, seqs, heads, kv_heads, packed, count),
        out_shape=[jax.ShapeDtypeStruct(*s) for s in shapes],
        in_specs=specs,
        out_specs=[VMEM] * len(shapes),
        scratch_shapes=scratch,
        compiler_params=pltpu.CompilerParams(vmem_limit_bytes=12 * MIB),
        name="hot_pages",
    )(*operands)


def project_kernel(received, seqs, heads, ways, z_ref, *refs):
    blocks = refs[:received]
    own_num, own_tot, hot_num, hot_tot, w_ref = refs[received : received + 5]
    outs = refs[received + 5 : received + 5 + ways]
    spread = refs[-1]
    head_dim = own_num.shape[1]
    rows = seqs // ways
    far = jnp.zeros((seqs, head_dim), jnp.float32)
    for b in blocks:
        far = far + b[heads].astype(jnp.float32)
    for h in range(heads):
        part = pl.ds(h * seqs, seqs)
        num = own_num[part, :] + hot_num[part, :]
        tot = own_tot[part, :] + hot_tot[part, :]
        for b in blocks:
            num = num + b[h].astype(jnp.float32)
        if blocks:
            tot = tot + (far[:, h : h + 1] + far[:, heads + h : heads + h + 1])
        spread[:, h * head_dim : (h + 1) * head_dim] = num / tot
    turned = []
    for k in range(ways):
        target = lax.rem(z_ref[0] + k, ways)
        turned.append(spread[pl.ds(pl.multiple_of(target * rows, rows), rows), :])
    att = jnp.concatenate(turned, axis=0).astype(jnp.bfloat16)
    model = w_ref.shape[1]
    tile = math.gcd(model, 768)
    for n in range(0, model, tile):
        res = dot_n(att, w_ref[:, n : n + tile])
        for k in range(ways):
            outs[k][:, n : n + tile] = res[k * rows : (k + 1) * rows].astype(outs[k].dtype)


def project(blocks, own, hot, o_weight, z, ways):
    head_dim = own[0].shape[1]
    width, model = o_weight.shape
    heads = width // head_dim
    seqs = hot[0].shape[0] // heads
    rows = seqs // ways
    kinds = [jnp.float32] + [jnp.bfloat16] * (ways - 1)
    return pl.pallas_call(
        functools.partial(project_kernel, len(blocks), seqs, heads, ways),
        out_shape=[jax.ShapeDtypeStruct((rows, model), kind) for kind in kinds],
        in_specs=[SMEM] + [VMEM] * (len(blocks) + 5),
        out_specs=[VMEM] * ways,
        scratch_shapes=[pltpu.VMEM((seqs, width), jnp.float32)],
        compiler_params=pltpu.CompilerParams(vmem_limit_bytes=8 * MIB),
        name="project",
    )(z, *blocks, *own, *hot, o_weight)


def norm_kernel(*refs):
    parts, (residual, gain, out) = refs[:-3], refs[-3:]
    projected = parts[0][...]
    for p in parts[1:]:
        projected = projected + p[...].astype(jnp.float32)
    mean_sq = jnp.mean(projected * projected, axis=1, keepdims=True)
    normed = projected / jnp.sqrt(mean_sq + epsilon) * gain[...]
    out[...] = (residual[...].astype(jnp.float32) + normed).astype(jnp.bfloat16)


def finish(parts, residual, norm_gain):
    return pl.pallas_call(
        norm_kernel,
        out_shape=jax.ShapeDtypeStruct(residual.shape, residual.dtype),
        compiler_params=pltpu.CompilerParams(vmem_limit_bytes=8 * MIB),
        name="finish",
    )(*parts, residual, norm_gain.reshape(1, -1))


def layer(
    chips, ways, queries, keys, values, hot_pages, hot_used, user_pages, lengths, o_weight, residual, norm_gain
):
    seqs, heads, head_dim = queries.shape
    page_count = keys.shape[0]
    me = lax.axis_index("pages")
    z = lax.axis_index("heads")
    devices = 2 * chips
    swap = [(i, i ^ 1) for i in range(devices)]
    power = chips & (chips - 1) == 0

    def there(i, k):
        return i ^ (2 * k) if power else (i + 2 * k) % devices

    q = queries.reshape(seqs * heads, head_dim)
    pages = user_pages.reshape(-1)
    out_perm = [[(i, there(i, k)) for i in range(devices)] for k in range(chips)]
    back_perm = [[(j, i) for i, j in perm] for perm in out_perm]
    own_kv = lead_pages(keys, values)
    partner_kv = tuple(lax.ppermute(x, "pages", swap) for x in own_kv)
    q, own_kv = lax.optimization_barrier((q, own_kv))
    late = [2] if chips > 2 else []
    soon = [k for k in reversed(range(1, chips)) if k not in late]
    far_q = {k: lax.ppermute(q, "pages", out_perm[k]) for k in soon + late}

    slot = jnp.arange(2 * HOT_CAP, dtype=jnp.int32)
    holder = jnp.where(slot < HOT_CAP, me, me ^ 1)
    page_ids = holder * page_count + slot % HOT_CAP
    matches = page_ids[:, None] == hot_pages[None, :]
    order = jnp.arange(hot_pages.shape[0], dtype=jnp.int32)
    absent = jnp.int32(jnp.iinfo(jnp.int32).max)
    position = jnp.min(jnp.where(matches, order[None, :], absent), axis=1)

    def used_of(k):
        origin = me ^ (2 * k) if power else lax.rem(me + devices - 2 * k, devices)
        row = lax.dynamic_slice_in_dim(hot_used, origin * seqs, seqs)
        return jnp.broadcast_to(row[:, None], (seqs, head_dim))

    used = [used_of(k) for k in range(chips)]
    turn, position, used = lax.optimization_barrier((z.reshape(1), position, used))
    *hot, own_k = hot_terms([q], [used[0]], position, own_kv, partner_kv, False, pages, keys)
    blocks = []
    own_v = None
    before = hot
    for ks in (soon, late):
        if not ks:
            continue
        before, arrived = lax.optimization_barrier((before, [far_q[k] for k in ks]))
        rest = (pages, values) if own_v is None else ()
        sent = hot_terms(arrived, [used[k] for k in ks], position, own_kv, partner_kv, True, *rest)
        if rest:
            *sent, own_v = sent
        for k, b in zip(ks, sent):
            blocks.append(lax.ppermute(b, "pages", back_perm[k]))
        before = sent
    if own_v is None:
        own_v = jnp.take(values, pages, axis=0)
    queries, before = lax.optimization_barrier((queries, before))
    own, weight = own_terms(queries, own_k, own_v, lengths, o_weight)
    parts = project(blocks, own, hot, weight, turn, ways)
    arrived = [parts[0]] + [
        lax.ppermute(parts[k], "heads", [(i, (i + k) % ways) for i in range(ways)])
        for k in range(1, ways)
    ]
    return finish(arrived, residual, norm_gain)


def solution(mesh):
    in_specs = (
        P("pages", "heads", None),
        P("pages", "heads", None, None),
        P("pages", "heads", None, None),
        P(),
        P(),
        P("pages", None),
        P("pages"),
        P("heads", None),
        P(("pages", "heads"), None),
        P(),
    )
    out_specs = P(("pages", "heads"), None)
    chips = mesh.shape["pages"] // 2
    body = functools.partial(layer, chips, mesh.shape["heads"])
    return jax.shard_map(body, mesh=mesh, in_specs=in_specs, out_specs=out_specs, check_vma=False)
```

```python
import functools
import math

import jax
import jax.numpy as jnp
from jax import lax
from jax.experimental import pallas as pl
from jax.experimental.pallas import tpu as pltpu
from jax.sharding import PartitionSpec as P


HOT_CAP = 8
score_scale = 1.0 / 12.0
soft_cap = 50.0
epsilon = 1e-06
inner = score_scale / soft_cap
outer = soft_cap * math.log2(math.e)
MIB = 1 << 20


def weights_of(logits):
    return jnp.exp2(outer * jnp.tanh(logits * inner))


def dot_t(a, b):
    return lax.dot_general(a, b, (((1,), (1,)), ((), ())), preferred_element_type=jnp.float32)


def dot_n(a, b):
    return lax.dot_general(a, b, (((1,), (0,)), ((), ())), preferred_element_type=jnp.float32)


def lead_kernel(keys_ref, values_ref, k_out, v_out, sems):
    copies = [
        pltpu.make_async_copy(src.at[pl.ds(0, dst.shape[0])], dst, sems.at[i])
        for i, (src, dst) in enumerate(((keys_ref, k_out), (values_ref, v_out)))
    ]
    for copy in copies:
        copy.start()
    for copy in copies:
        copy.wait()


def in_hbm(x):
    return pltpu.with_memory_space_constraint(x, pltpu.HBM)


HBM = pl.BlockSpec(memory_space=pltpu.HBM)
VMEM = pl.BlockSpec(memory_space=pltpu.VMEM)
SMEM = pl.BlockSpec(memory_space=pltpu.SMEM)


def lead_pages(keys, values):
    out = jax.ShapeDtypeStruct((HOT_CAP, *keys.shape[1:]), keys.dtype)
    return pl.pallas_call(
        lead_kernel,
        out_shape=(out, out),
        in_specs=[HBM, HBM],
        out_specs=(VMEM, VMEM),
        scratch_shapes=[pltpu.SemaphoreType.DMA((2,))],
        compiler_params=pltpu.CompilerParams(vmem_limit_bytes=4 * MIB),
        name="lead_pages",
    )(in_hbm(keys), in_hbm(values))


def own_kernel(
    seqs, ups, heads, group, kv_heads,
    lengths_ref, q_ref, kbuf, *refs,
):
    *vbufs, w_hbm, num_ref, tot_ref, w_ref, sem = refs
    page_len, head_dim = kbuf.shape[2], kbuf.shape[3]
    width = kv_heads * page_len
    prefetch = pltpu.make_async_copy(w_hbm, w_ref, sem)
    prefetch.start()
    column = lax.broadcasted_iota(jnp.int32, (heads, width), 1)
    row = lax.broadcasted_iota(jnp.int32, (heads, width), 0)
    mine = (column // page_len) == (row // group)
    token = jnp.where(mine, column % page_len, ups * page_len)
    ones = jnp.ones((width, head_dim), jnp.bfloat16)

    done = 0
    for vbuf in vbufs:
        part = vbuf.shape[0] // ups
        unroll = math.gcd(part, 16)

        def block(b, carry, first=done, unroll=unroll, vbuf=vbuf):
            for j in range(unroll):
                at = b * unroll + j
                s = first + at
                q = q_ref[pl.ds(pl.multiple_of(s * heads, heads), heads), :]
                total = jnp.zeros((heads, 2 * head_dim), jnp.float32)
                for u in range(ups):
                    k = kbuf[s * ups + u].reshape(width, head_dim)
                    v = vbuf[at * ups + u].reshape(width, head_dim)
                    allowed = token < lengths_ref[s] - u * page_len
                    weight = jnp.where(allowed, weights_of(dot_t(q, k)), 0.0).astype(jnp.bfloat16)
                    total = total + dot_n(weight, jnp.concatenate([v, ones], axis=1))
                num_ref[pl.ds(s, heads, stride=seqs), :] = total[:, :head_dim]
                tot_ref[pl.ds(s, heads, stride=seqs), :] = total[:, head_dim:]
            return carry

        lax.fori_loop(0, part // unroll, block, 0)
        done += part
    prefetch.wait()


def own_terms(q, own_k, own_v, lengths, o_weight):
    seqs, _, head_dim = q.shape
    count, kv_heads, _, _ = own_k.shape
    group = q.shape[1] // kv_heads
    heads = -(-q.shape[1] // 8) * 8
    q = jnp.pad(q, ((0, 0), (0, heads - q.shape[1]), (0, 0))).reshape(seqs * heads, head_dim)
    out = jax.ShapeDtypeStruct((heads * seqs, head_dim), jnp.float32)
    num, tot, w = pl.pallas_call(
        functools.partial(own_kernel, seqs, count // seqs, heads, group, kv_heads),
        out_shape=(out, out, jax.ShapeDtypeStruct(o_weight.shape, o_weight.dtype)),
        in_specs=[SMEM, VMEM, VMEM] + [VMEM] * len(own_v) + [HBM],
        out_specs=(VMEM, VMEM, VMEM),
        scratch_shapes=[pltpu.SemaphoreType.DMA],
        compiler_params=pltpu.CompilerParams(vmem_limit_bytes=8 * MIB),
        name="own_pages",
    )(lengths, q, own_k, *own_v, in_hbm(o_weight))
    return (num, tot), w


def shared_places(me, cap, page_count, hot_ref, lanes):
    shape = (2 * cap, hot_ref.shape[1])
    slot = lax.broadcasted_iota(jnp.int32, shape, 0)
    lane = lax.broadcasted_iota(jnp.int32, shape, 1).astype(jnp.float32)
    first = jnp.where(slot < cap, me * page_count, (me ^ 1) * page_count - cap)
    matches = jnp.broadcast_to(hot_ref[...], shape) == first + slot
    place = jnp.min(jnp.where(matches, lane, 1e9), axis=1, keepdims=True)
    return jnp.broadcast_to(place, (2 * cap, lanes))


def used_column(origin, seqs, used_ref, lanes):
    span = used_ref.shape[1]
    row = used_ref[pl.ds(origin * seqs // span, 1), :].astype(jnp.float32)
    shape = (seqs, span)
    lane = lax.broadcasted_iota(jnp.int32, shape, 1)
    sequence = lax.broadcasted_iota(jnp.int32, shape, 0) + origin * seqs % span
    picked = jnp.where(lane == sequence, jnp.broadcast_to(row, shape), 0.0)
    return jnp.broadcast_to(jnp.sum(picked, axis=1, keepdims=True), (seqs, lanes))


def hot_kernel(
    sources, seqs, heads, kv_heads, packed, fetch, shifts, page_count, hot_ref, used_ref, *refs
):
    if fetch:
        pages_ref, cache_ref, *refs = refs
        *refs, pages_out, staged, places, sems = refs

        def copy(i):
            return pltpu.make_async_copy(cache_ref.at[pages_ref[i]], pages_out.at[i], sems.at[i])

        def start(i, carry):
            copy(i).start()
            return carry

        def wait(i, carry):
            copy(i).wait()
            return carry

        lax.fori_loop(0, fetch, start, 0)
    else:
        *refs, staged, places = refs
    queries = refs[:sources]
    halves = (refs[sources : sources + 2], refs[sources + 2 : sources + 4])
    outs = refs[sources + 4 :]
    group = heads // kv_heads
    cap, _, page_len, head_dim = halves[0][0].shape
    lane = lax.broadcasted_iota(jnp.int32, (seqs, head_dim), 1)
    for r in range(sources):
        staged[r] = queries[r][...].astype(jnp.float32)
    me = lax.axis_index("pages")
    places[...] = shared_places(me, cap, page_count, hot_ref, head_dim)
    used_rows = [used_column(shift(me), seqs, used_ref, head_dim) for shift in shifts]
    step = 2
    ones = jnp.ones((step * page_len, head_dim), jnp.bfloat16)
    totals = [jnp.zeros((seqs, head_dim), jnp.float32) for _ in range(sources)]
    for h in range(kv_heads):
        rows = [
            staged[r, pl.ds(h * group + g, seqs, stride=heads), :].astype(jnp.bfloat16)
            for r in range(sources)
            for g in range(group)
        ]
        q = jnp.concatenate(rows, axis=0)
        acc = jnp.zeros((q.shape[0], 2 * head_dim), jnp.float32)
        for half, (k_ref, v_ref) in enumerate(halves):
            for c in range(0, cap, step):
                k = k_ref[c : c + step, h].reshape(step * page_len, head_dim)
                v = v_ref[c : c + step, h].reshape(step * page_len, head_dim)
                weight = weights_of(dot_t(q, k))
                parts = []
                for p in range(step):
                    slot = half * cap + c + p
                    place = jnp.broadcast_to(places[slot : slot + 1, :], (seqs, page_len))
                    columns = slice(p * page_len, (p + 1) * page_len)
                    part = []
                    for r in range(sources):
                        mask = used_rows[r] > place
                        for i in range(r * group, (r + 1) * group):
                            part.append(jnp.where(mask, weight[i * seqs : (i + 1) * seqs, columns], 0.0))
                    parts.append(jnp.concatenate(part, axis=0).astype(jnp.bfloat16))
                acc = acc + dot_n(jnp.concatenate(parts, axis=1), jnp.concatenate([v, ones], axis=1))
        for r in range(sources):
            for g in range(group):
                i = r * group + g
                head = h * group + g
                num = acc[i * seqs : (i + 1) * seqs, :head_dim]
                tot = acc[i * seqs : (i + 1) * seqs, head_dim:]
                if packed:
                    rest = tot - tot.astype(jnp.bfloat16).astype(jnp.float32)
                    outs[r][head] = num.astype(jnp.bfloat16)
                    low = jnp.where(lane == heads + head, rest, totals[r])
                    totals[r] = jnp.where(lane == head, tot, low)
                else:
                    outs[2 * r][head * seqs : (head + 1) * seqs, :] = num
                    outs[2 * r + 1][head * seqs : (head + 1) * seqs, :] = tot
    if packed:
        for r in range(sources):
            outs[r][heads] = totals[r].astype(jnp.bfloat16)
    if fetch:
        lax.fori_loop(0, fetch, wait, 0)


def hot_terms(queries, shifts, page_count, tables, own_kv, partner_kv, packed, fetch=()):
    sources = len(queries)
    _, kv_heads, page_len, head_dim = own_kv[0].shape
    seqs, heads = queries[0].shape[:2]
    if packed:
        shapes = [((heads + 1, seqs, head_dim), jnp.bfloat16)] * sources
    else:
        shapes = [((heads * seqs, head_dim), jnp.float32)] * (2 * sources)
    scratch = [
        pltpu.VMEM((sources, seqs * heads, head_dim), jnp.float32),
        pltpu.VMEM((2 * HOT_CAP, head_dim), jnp.float32),
    ]
    flat = [q.reshape(seqs * heads, head_dim) for q in queries]
    operands = [*tables, *flat, *own_kv, *partner_kv]
    specs = [VMEM] * len(operands)
    count = 0
    if fetch:
        pages, cache = fetch
        count = pages.shape[0]
        operands[2:2] = [pages, in_hbm(cache)]
        specs[2:2] = [SMEM, HBM]
        shapes.append(((count, kv_heads, page_len, head_dim), cache.dtype))
        scratch.append(pltpu.SemaphoreType.DMA((count,)))
    return pl.pallas_call(
        functools.partial(
            hot_kernel, sources, seqs, heads, kv_heads, packed, count, shifts, page_count
        ),
        out_shape=[jax.ShapeDtypeStruct(*s) for s in shapes],
        in_specs=specs,
        out_specs=[VMEM] * len(shapes),
        scratch_shapes=scratch,
        compiler_params=pltpu.CompilerParams(vmem_limit_bytes=12 * MIB),
        name="hot_pages",
    )(*operands)


def row_owner(i, k, ways):
    return i ^ k if ways & (ways - 1) == 0 else lax.rem(i + k, ways)


def row_order(ways):
    return [2, 3, 1] if ways == 4 else list(range(ways - 1, 0, -1))


def project_kernel(received, seqs, heads, ways, *refs):
    blocks = refs[:received]
    own_num, own_tot, hot_num, hot_tot, w_ref = refs[received : received + 5]
    outs = refs[received + 5 : received + 5 + ways]
    spread = refs[-1]
    head_dim = own_num.shape[1]
    rows = seqs // ways
    far = jnp.zeros((seqs, head_dim), jnp.float32)
    for b in blocks:
        far = far + b[heads].astype(jnp.float32)
    for h in range(heads):
        part = pl.ds(h * seqs, seqs)
        num = own_num[part, :] + hot_num[part, :]
        tot = own_tot[part, :] + hot_tot[part, :]
        for b in blocks:
            num = num + b[h].astype(jnp.float32)
        if blocks:
            tot = tot + (far[:, h : h + 1] + far[:, heads + h : heads + h + 1])
        spread[:, h * head_dim : (h + 1) * head_dim] = num / tot
    turned = []
    for k in range(ways):
        target = row_owner(lax.axis_index("heads"), k, ways)
        turned.append(spread[pl.ds(pl.multiple_of(target * rows, rows), rows), :])
    att = jnp.concatenate(turned, axis=0).astype(jnp.bfloat16)
    model = w_ref.shape[1]
    tile = math.gcd(model, 768)
    for n in range(0, model, tile):
        res = dot_n(att, w_ref[:, n : n + tile])
        for k in range(ways):
            outs[k][:, n : n + tile] = res[k * rows : (k + 1) * rows].astype(outs[k].dtype)


def project(blocks, own, hot, o_weight, ways):
    head_dim = own[0].shape[1]
    width, model = o_weight.shape
    heads = width // head_dim
    seqs = hot[0].shape[0] // heads
    rows = seqs // ways
    kinds = [jnp.float32] + [jnp.bfloat16] * (ways - 1)
    return pl.pallas_call(
        functools.partial(project_kernel, len(blocks), seqs, heads, ways),
        out_shape=[jax.ShapeDtypeStruct((rows, model), kind) for kind in kinds],
        in_specs=[VMEM] * (len(blocks) + 5),
        out_specs=[VMEM] * ways,
        scratch_shapes=[pltpu.VMEM((seqs, width), jnp.float32)],
        compiler_params=pltpu.CompilerParams(vmem_limit_bytes=8 * MIB),
        name="project",
    )(*blocks, *own, *hot, o_weight)


def norm_kernel(*refs):
    parts, (residual, gain, out) = refs[:-3], refs[-3:]
    projected = parts[0][...]
    for p in parts[1:]:
        projected = projected + p[...].astype(jnp.float32)
    mean_sq = jnp.mean(projected * projected, axis=1, keepdims=True)
    normed = projected / jnp.sqrt(mean_sq + epsilon) * gain[...]
    out[...] = (residual[...].astype(jnp.float32) + normed).astype(jnp.bfloat16)


def finish(parts, residual, norm_gain):
    return pl.pallas_call(
        norm_kernel,
        out_shape=jax.ShapeDtypeStruct(residual.shape, residual.dtype),
        compiler_params=pltpu.CompilerParams(vmem_limit_bytes=8 * MIB),
        name="finish",
    )(*parts, residual, norm_gain.reshape(1, -1))


def layer(
    chips, ways, queries, keys, values, hot_pages, hot_used, user_pages, lengths, o_weight, residual, norm_gain
):
    page_count = keys.shape[0]
    devices = 2 * chips
    swap = [(i, i ^ 1) for i in range(devices)]
    power = chips & (chips - 1) == 0

    def there(i, k):
        return i ^ (2 * k) if power else (i + 2 * k) % devices

    pages = user_pages.reshape(-1)
    out_perm = [[(i, there(i, k)) for i in range(devices)] for k in range(chips)]
    back_perm = [[(j, i) for i, j in perm] for perm in out_perm]
    own_kv = lead_pages(keys, values)
    partner_kv = tuple(lax.ppermute(x, "pages", swap) for x in own_kv)
    q, own_kv = lax.optimization_barrier((queries, own_kv))
    late = [chips - 1] if chips > 2 else []
    soon = [k for k in range(1, chips) if k not in late]
    far_q = {}
    for k in soon + late:
        far_q[k] = lax.ppermute(q, "pages", out_perm[k])

    def shift(k):
        if power:
            return lambda i: i ^ (2 * k)
        return lambda i: lax.rem(i + devices - 2 * k, devices)

    tables = (hot_pages.reshape(1, -1), hot_used.reshape(-1, 128))
    *hot, own_k = hot_terms(
        [queries], [shift(0)], page_count, tables, own_kv, partner_kv, False, (pages, keys)
    )
    groups = [ks for ks in (soon, late) if ks]
    blocks, own_v = [], []
    before = hot
    half = pages.shape[0] // 2 if len(groups) == 2 else pages.shape[0]
    for n, ks in enumerate(groups):
        before, arrived = lax.optimization_barrier((before, [far_q[k] for k in ks]))
        fetch = (pages[n * half : (n + 1) * half], values)
        *sent, part = hot_terms(
            arrived, [shift(k) for k in ks], page_count, tables, own_kv, partner_kv, True, fetch
        )
        own_v.append(part)
        for k, b in zip(ks, sent):
            blocks.append(lax.ppermute(b, "pages", back_perm[k]))
        before = sent
    if not groups:
        own_v = [jnp.take(values, pages, axis=0)]
    queries, before = lax.optimization_barrier((queries, before))
    own, weight = own_terms(queries, own_k, own_v, lengths, o_weight)
    parts = project(blocks, own, hot, weight, ways)
    arrived = [parts[0]]
    for k in row_order(ways):
        pairs = [(i, i ^ k if ways & (ways - 1) == 0 else (i + k) % ways) for i in range(ways)]
        arrived.append(lax.ppermute(parts[k], "heads", pairs))
    return finish(arrived, residual, norm_gain)


def solution(mesh):
    in_specs = (
        P("pages", "heads", None),
        P("pages", "heads", None, None),
        P("pages", "heads", None, None),
        P(),
        P(),
        P("pages", None),
        P("pages"),
        P("heads", None),
        P(("pages", "heads"), None),
        P(),
    )
    out_specs = P(("pages", "heads"), None)
    chips = mesh.shape["pages"] // 2
    body = functools.partial(layer, chips, mesh.shape["heads"])
    return jax.shard_map(body, mesh=mesh, in_specs=in_specs, out_specs=out_specs, check_vma=False)
```

```python
import functools
import math

import jax
import jax.numpy as jnp
from jax import lax
from jax.experimental import pallas as pl
from jax.experimental.pallas import tpu as pltpu
from jax.sharding import PartitionSpec as P


HOT_CAP = 8
score_scale = 1.0 / 12.0
soft_cap = 50.0
epsilon = 1e-06
inner = score_scale / soft_cap
outer = soft_cap * math.log2(math.e)
MIB = 1 << 20


def weights_of(logits):
    return jnp.exp2(outer * jnp.tanh(logits * inner))


def dot_t(a, b):
    return lax.dot_general(a, b, (((1,), (1,)), ((), ())), preferred_element_type=jnp.float32)


def dot_n(a, b):
    return lax.dot_general(a, b, (((1,), (0,)), ((), ())), preferred_element_type=jnp.float32)


def lead_kernel(keys_ref, values_ref, k_out, v_out, sems):
    copies = [
        pltpu.make_async_copy(src.at[pl.ds(0, dst.shape[0])], dst, sems.at[i])
        for i, (src, dst) in enumerate(((keys_ref, k_out), (values_ref, v_out)))
    ]
    for copy in copies:
        copy.start()
    for copy in copies:
        copy.wait()


def in_hbm(x):
    return pltpu.with_memory_space_constraint(x, pltpu.HBM)


HBM = pl.BlockSpec(memory_space=pltpu.HBM)
VMEM = pl.BlockSpec(memory_space=pltpu.VMEM)
SMEM = pl.BlockSpec(memory_space=pltpu.SMEM)


def lead_pages(keys, values):
    out = jax.ShapeDtypeStruct((HOT_CAP, *keys.shape[1:]), keys.dtype)
    return pl.pallas_call(
        lead_kernel,
        out_shape=(out, out),
        in_specs=[HBM, HBM],
        out_specs=(VMEM, VMEM),
        scratch_shapes=[pltpu.SemaphoreType.DMA((2,))],
        compiler_params=pltpu.CompilerParams(vmem_limit_bytes=4 * MIB),
        name="lead_pages",
    )(in_hbm(keys), in_hbm(values))


def own_kernel(
    seqs, ups, heads, group, kv_heads,
    pages_ref, lengths_ref, q_ref, first_k, last_k, first_v, v_hbm, w_hbm,
    num_ref, tot_ref, w_ref, last_v, sem, tail_sem,
):
    page_len, head_dim = first_v.shape[2:]
    early, late = first_k.shape[0], last_k.shape[0]

    def tail(act):
        def one(i, carry):
            act(pltpu.make_async_copy(v_hbm.at[pages_ref[early + i]], last_v.at[i], tail_sem.at[i]))
            return carry

        lax.fori_loop(0, late, one, 0)

    tail(lambda copy: copy.start())
    width = kv_heads * page_len
    prefetch = pltpu.make_async_copy(w_hbm, w_ref, sem)
    prefetch.start()
    column = lax.broadcasted_iota(jnp.int32, (heads, width), 1)
    row = lax.broadcasted_iota(jnp.int32, (heads, width), 0)
    mine = (column // page_len) == (row // group)
    token = jnp.where(mine, column % page_len, ups * page_len)
    ones = jnp.ones((width, head_dim), jnp.bfloat16)
    done = 0
    for kbuf, vbuf in ((first_k, first_v), (last_k, last_v)):
        if kbuf is last_k:
            tail(lambda copy: copy.wait())
        part = kbuf.shape[0] // ups
        unroll = math.gcd(part, 16)

        def block(b, carry, first=done, unroll=unroll, kbuf=kbuf, vbuf=vbuf):
            for j in range(unroll):
                at = b * unroll + j
                s = first + at
                q = q_ref[pl.ds(pl.multiple_of(s * heads, heads), heads), :]
                total = jnp.zeros((heads, 2 * head_dim), jnp.float32)
                for u in range(ups):
                    k = kbuf[at * ups + u].reshape(width, head_dim)
                    v = vbuf[at * ups + u].reshape(width, head_dim)
                    allowed = token < lengths_ref[s] - u * page_len
                    weight = jnp.where(allowed, weights_of(dot_t(q, k)), 0.0).astype(jnp.bfloat16)
                    total = total + dot_n(weight, jnp.concatenate([v, ones], axis=1))
                num_ref[pl.ds(s, heads, stride=seqs), :] = total[:, :head_dim]
                tot_ref[pl.ds(s, heads, stride=seqs), :] = total[:, head_dim:]
            return carry

        lax.fori_loop(0, part // unroll, block, 0)
        done += part
    prefetch.wait()


def own_terms(q, pages, own_k, first_v, values, lengths, o_weight):
    seqs, _, head_dim = q.shape
    _, kv_heads, page_len, _ = first_v.shape
    count, late = pages.shape[0], own_k[1].shape[0]
    group = q.shape[1] // kv_heads
    heads = -(-q.shape[1] // 8) * 8
    q = jnp.pad(q, ((0, 0), (0, heads - q.shape[1]), (0, 0))).reshape(seqs * heads, head_dim)
    out = jax.ShapeDtypeStruct((heads * seqs, head_dim), jnp.float32)
    num, tot, w = pl.pallas_call(
        functools.partial(own_kernel, seqs, count // seqs, heads, group, kv_heads),
        out_shape=(out, out, jax.ShapeDtypeStruct(o_weight.shape, o_weight.dtype)),
        in_specs=[SMEM, SMEM] + [VMEM] * 4 + [HBM, HBM],
        out_specs=(VMEM, VMEM, VMEM),
        scratch_shapes=[
            pltpu.VMEM((late, kv_heads, page_len, head_dim), values.dtype),
            pltpu.SemaphoreType.DMA,
            pltpu.SemaphoreType.DMA((late,)),
        ],
        compiler_params=pltpu.CompilerParams(vmem_limit_bytes=8 * MIB),
        name="own_pages",
    )(pages, lengths, q, *own_k, first_v, in_hbm(values), in_hbm(o_weight))
    return (num, tot), w


def shared_places(me, cap, page_count, hot_ref, lanes):
    shape = (2 * cap, hot_ref.shape[1])
    slot = lax.broadcasted_iota(jnp.int32, shape, 0)
    lane = lax.broadcasted_iota(jnp.int32, shape, 1).astype(jnp.float32)
    first = jnp.where(slot < cap, me * page_count, (me ^ 1) * page_count - cap)
    matches = jnp.broadcast_to(hot_ref[...], shape) == first + slot
    place = jnp.min(jnp.where(matches, lane, 1e9), axis=1, keepdims=True)
    return jnp.broadcast_to(place, (2 * cap, lanes))


def used_column(origin, seqs, used_ref, lanes):
    span = used_ref.shape[1]
    row = used_ref[pl.ds(origin * seqs // span, 1), :].astype(jnp.float32)
    shape = (seqs, span)
    lane = lax.broadcasted_iota(jnp.int32, shape, 1)
    sequence = lax.broadcasted_iota(jnp.int32, shape, 0) + origin * seqs % span
    picked = jnp.where(lane == sequence, jnp.broadcast_to(row, shape), 0.0)
    return jnp.broadcast_to(jnp.sum(picked, axis=1, keepdims=True), (seqs, lanes))


def hot_kernel(sources, halves, seqs, heads, kv_heads, fetches, page_count, hot_ref, used_ref, *refs):
    pages_ref, *refs = refs
    jobs = len(fetches)
    caches, refs = refs[:jobs], refs[jobs:]
    refs, fetched, (staged, places), sems = (
        refs[: -2 * jobs - 2], refs[-2 * jobs - 2 : -jobs - 2], refs[-jobs - 2 : -jobs], refs[-jobs:]
    )

    def each(act):
        for n, (first, last) in enumerate(fetches):

            def one(i, carry, n=n, first=first):
                src = caches[n].at[pages_ref[first + i]]
                act(pltpu.make_async_copy(src, fetched[n].at[i], sems[n].at[i]))
                return carry

            lax.fori_loop(0, last - first, one, 0)

    each(lambda copy: copy.start())
    count = len(sources)
    queries, refs = refs[:count], refs[count:]
    kv = [(refs[2 * i], refs[2 * i + 1]) for i in range(len(halves))]
    outs = list(refs[2 * len(halves) :])
    group = heads // kv_heads
    cap, _, page_len, head_dim = kv[0][0].shape
    lane = lax.broadcasted_iota(jnp.int32, (8, head_dim), 1)
    for r in range(count):
        staged[r] = queries[r][...].astype(jnp.float32)
    me = lax.axis_index("pages")
    places[...] = shared_places(me, cap, page_count, hot_ref, head_dim)
    used_rows = [used_column(shift(me), seqs, used_ref, head_dim) for shift, _, _ in sources]
    step = 2
    ones = jnp.ones((step * page_len, head_dim), jnp.bfloat16)
    dests = []
    for _, _, packed in sources:
        dests.append(outs.pop(0) if packed else (outs.pop(0), outs.pop(0)))
    totals = [jnp.zeros((8, head_dim), jnp.float32) for _ in range(count)]
    for h in range(kv_heads):
        rows = [
            [
                staged[r, pl.ds(h * group + g, seqs, stride=heads), :].astype(jnp.bfloat16)
                for g in range(group)
            ]
            for r in range(count)
        ]
        acc = [jnp.zeros((group * seqs, 2 * head_dim), jnp.float32) for _ in range(count)]
        for half, (k_ref, v_ref) in zip(halves, kv):
            active = [r for r in range(count) if half in sources[r][1]]
            q = jnp.concatenate([row for r in active for row in rows[r]], axis=0)
            for c in range(0, cap, step):
                k = k_ref[c : c + step, h].reshape(step * page_len, head_dim)
                v = v_ref[c : c + step, h].reshape(step * page_len, head_dim)
                weight = weights_of(dot_t(q, k))
                parts = []
                for p in range(step):
                    slot = half * cap + c + p
                    place = jnp.broadcast_to(places[slot : slot + 1, :], (seqs, page_len))
                    columns = slice(p * page_len, (p + 1) * page_len)
                    part = []
                    for n, r in enumerate(active):
                        mask = used_rows[r] > place
                        for i in range(n * group, (n + 1) * group):
                            part.append(jnp.where(mask, weight[i * seqs : (i + 1) * seqs, columns], 0.0))
                    parts.append(jnp.concatenate(part, axis=0).astype(jnp.bfloat16))
                res = dot_n(jnp.concatenate(parts, axis=1), jnp.concatenate([v, ones], axis=1))
                for n, r in enumerate(active):
                    acc[r] = acc[r] + res[n * group * seqs : (n + 1) * group * seqs]
        for r, (_, _, packed) in enumerate(sources):
            for g in range(group):
                head = h * group + g
                num = acc[r][g * seqs : (g + 1) * seqs, :head_dim]
                tot = acc[r][g * seqs : (g + 1) * seqs, head_dim:]
                if packed:
                    rest = tot - tot.astype(jnp.bfloat16).astype(jnp.float32)
                    dests[r][head * seqs : (head + 1) * seqs, :] = num.astype(jnp.bfloat16)
                    for j in range(seqs // 8):
                        at, fold = 2 * heads * j + head, slice(8 * j, 8 * j + 8)
                        low = jnp.where(lane == at + heads, rest[fold], totals[r])
                        totals[r] = jnp.where(lane == at, tot[fold], low)
                else:
                    dests[r][0][head * seqs : (head + 1) * seqs, :] = num
                    dests[r][1][head * seqs : (head + 1) * seqs, :] = tot
    for r, (_, _, packed) in enumerate(sources):
        if packed:
            padded = jnp.concatenate([totals[r], jnp.zeros_like(totals[r])], axis=0)
            dests[r][heads * seqs :, :] = padded.astype(jnp.bfloat16)
    each(lambda copy: copy.wait())


def hot_terms(queries, sources, halves, kv, page_count, tables, pages, fetch):
    _, kv_heads, page_len, head_dim = kv[0].shape
    seqs, heads = queries[0].shape[:2]
    shapes = []
    for _, _, packed in sources:
        if packed:
            shapes.append(((heads * seqs + 16, head_dim), jnp.bfloat16))
        else:
            shapes += [((heads * seqs, head_dim), jnp.float32)] * 2
    counts = [last - first for _, first, last in fetch]
    shapes += [((n, kv_heads, page_len, head_dim), kv[0].dtype) for n in counts]
    fetches = tuple((first, last) for _, first, last in fetch)
    flat = [q.reshape(seqs * heads, head_dim) for q in queries]
    operands = [*tables, pages, *(in_hbm(f[0]) for f in fetch), *flat, *kv]
    return pl.pallas_call(
        functools.partial(
            hot_kernel, sources, halves, seqs, heads, kv_heads, fetches, page_count
        ),
        out_shape=[jax.ShapeDtypeStruct(*s) for s in shapes],
        in_specs=[VMEM, VMEM, SMEM] + [HBM] * len(fetch) + [VMEM] * (len(flat) + len(kv)),
        out_specs=[VMEM] * len(shapes),
        scratch_shapes=[
            pltpu.VMEM((len(sources), seqs * heads, head_dim), jnp.float32),
            pltpu.VMEM((2 * HOT_CAP, head_dim), jnp.float32),
            *(pltpu.SemaphoreType.DMA((n,)) for n in counts),
        ],
        compiler_params=pltpu.CompilerParams(vmem_limit_bytes=12 * MIB),
        name="hot_pages",
    )(*operands)


def row_owner(i, k, ways):
    return i ^ k if ways & (ways - 1) == 0 else lax.rem(i + k, ways)


def row_order(ways):
    return [2, 1, 3] if ways == 4 else list(range(ways - 1, 0, -1))


def project_kernel(received, seqs, heads, ways, *refs):
    blocks = refs[:received]
    nums, tots = refs[received : received + 3], refs[received + 3 : received + 6]
    w_ref, outs, spread = refs[received + 6], refs[received + 7 : received + 7 + ways], refs[-1]
    head_dim = nums[0].shape[1]
    rows = seqs // ways
    far = jnp.zeros((16, head_dim), jnp.float32)
    for b in blocks:
        far = far + b[heads * seqs :, :].astype(jnp.float32)
    for h in range(heads):
        part = pl.ds(h * seqs, seqs)
        num = nums[0][part, :] + nums[1][part, :] + nums[2][part, :]
        tot = tots[0][part, :] + tots[1][part, :] + tots[2][part, :]
        for b in blocks:
            num = num + b[part, :].astype(jnp.float32)
        if blocks:
            folds = []
            for at in range(h, 2 * heads * (seqs // 8), 2 * heads):
                fold = far[:8, at : at + 1] + far[:8, at + heads : at + heads + 1]
                folds.append(jnp.broadcast_to(fold, (8, head_dim)))
            tot = tot + jnp.concatenate(folds, axis=0)
        spread[:, h * head_dim : (h + 1) * head_dim] = num / tot
    turned = []
    for k in range(ways):
        target = row_owner(lax.axis_index("heads"), k, ways)
        turned.append(spread[pl.ds(pl.multiple_of(target * rows, rows), rows), :])
    att = jnp.concatenate(turned, axis=0).astype(jnp.bfloat16)
    model = w_ref.shape[1]
    tile = math.gcd(model, 768)
    for n in range(0, model, tile):
        res = dot_n(att, w_ref[:, n : n + tile])
        for k in range(ways):
            outs[k][:, n : n + tile] = res[k * rows : (k + 1) * rows].astype(outs[k].dtype)


def project(blocks, near, rest, own, o_weight, ways):
    head_dim = own[0].shape[1]
    width, model = o_weight.shape
    heads = width // head_dim
    seqs = near[0].shape[0] // heads
    rows = seqs // ways
    kinds = [jnp.float32] + [jnp.bfloat16] * (ways - 1)
    return pl.pallas_call(
        functools.partial(project_kernel, len(blocks), seqs, heads, ways),
        out_shape=[jax.ShapeDtypeStruct((rows, model), kind) for kind in kinds],
        in_specs=[VMEM] * (len(blocks) + 7),
        out_specs=[VMEM] * ways,
        scratch_shapes=[pltpu.VMEM((seqs, width), jnp.float32)],
        compiler_params=pltpu.CompilerParams(vmem_limit_bytes=8 * MIB),
        name="project",
    )(*blocks, near[0], rest[0], own[0], near[1], rest[1], own[1], o_weight)


def norm_kernel(*refs):
    parts, (residual, gain, out) = refs[:-3], refs[-3:]
    projected = parts[0][...]
    for p in parts[1:]:
        projected = projected + p[...].astype(jnp.float32)
    mean_sq = jnp.mean(projected * projected, axis=1, keepdims=True)
    normed = projected / jnp.sqrt(mean_sq + epsilon) * gain[...]
    out[...] = (residual[...].astype(jnp.float32) + normed).astype(jnp.bfloat16)


def finish(parts, residual, norm_gain):
    return pl.pallas_call(
        norm_kernel,
        out_shape=jax.ShapeDtypeStruct(residual.shape, residual.dtype),
        compiler_params=pltpu.CompilerParams(vmem_limit_bytes=8 * MIB),
        name="finish",
    )(*parts, residual, norm_gain.reshape(1, -1))


def layer(
    chips, ways, queries, keys, values, hot_pages, hot_used, user_pages, lengths, o_weight, residual, norm_gain
):
    page_count = keys.shape[0]
    devices = 2 * chips
    swap = [(i, i ^ 1) for i in range(devices)]
    power = chips & (chips - 1) == 0

    def there(i, k):
        return i ^ (2 * k) if power else (i + 2 * k) % devices

    pages = user_pages.reshape(-1)
    out_perm = [[(i, there(i, k)) for i in range(devices)] for k in range(chips)]
    back_perm = [[(j, i) for i, j in perm] for perm in out_perm]
    far_q = []
    for k in range(1, chips):
        far_q.append(lax.ppermute(queries, "pages", out_perm[k]))
    own_kv = lead_pages(keys, values)
    partner_kv = tuple(lax.ppermute(x, "pages", swap) for x in own_kv)

    def shift(k):
        if power:
            return lambda i: i ^ (2 * k)
        return lambda i: lax.rem(i + devices - 2 * k, devices)

    tables = (hot_pages.reshape(1, -1), hot_used.reshape(-1, 128))
    count = pages.shape[0]
    early = count // 4 * 3 // user_pages.shape[1] * user_pages.shape[1]
    *near, first_k = hot_terms(
        [queries], [(shift(0), (0,), False)], (0,), own_kv, page_count, tables, pages,
        [(keys, 0, early)],
    )
    near, far_q, partner_kv = lax.optimization_barrier((near, far_q, partner_kv))
    sources = [(shift(k), (0, 1), True) for k in range(1, chips)] + [(shift(0), (1,), False)]
    *sent, rest_num, rest_tot, last_k, first_v = hot_terms(
        [*far_q, queries], sources, (0, 1), (*own_kv, *partner_kv), page_count, tables, pages,
        [(keys, early, count), (values, 0, early)],
    )
    blocks = []
    for k, b in zip(range(1, chips), sent):
        blocks.append(lax.ppermute(b, "pages", back_perm[k]))
    queries, rest_num = lax.optimization_barrier((queries, rest_num))
    own, weight = own_terms(queries, pages, (first_k, last_k), first_v, values, lengths, o_weight)
    parts = project(blocks, near, (rest_num, rest_tot), own, weight, ways)
    arrived = [parts[0]]
    for k in row_order(ways):
        pairs = [(i, i ^ k if ways & (ways - 1) == 0 else (i + k) % ways) for i in range(ways)]
        arrived.append(lax.ppermute(parts[k], "heads", pairs))
    return finish(arrived, residual, norm_gain)


def solution(mesh):
    in_specs = (
        P("pages", "heads", None),
        P("pages", "heads", None, None),
        P("pages", "heads", None, None),
        P(),
        P(),
        P("pages", None),
        P("pages"),
        P("heads", None),
        P(("pages", "heads"), None),
        P(),
    )
    out_specs = P(("pages", "heads"), None)
    chips = mesh.shape["pages"] // 2
    body = functools.partial(layer, chips, mesh.shape["heads"])
    return jax.shard_map(body, mesh=mesh, in_specs=in_specs, out_specs=out_specs, check_vma=False)
```

```python
import functools
import math

import jax
import jax.numpy as jnp
from jax import lax
from jax.experimental import pallas as pl
from jax.experimental.pallas import tpu as pltpu
from jax.sharding import PartitionSpec as P


HOT_CAP = 8
score_scale = 1.0 / 12.0
soft_cap = 50.0
epsilon = 1e-06
inner = score_scale / soft_cap
outer = soft_cap * math.log2(math.e)
MIB = 1 << 20


def weights_of(logits):
    return jnp.exp2(outer * jnp.tanh(logits * inner))


def dot_t(a, b):
    return lax.dot_general(a, b, (((1,), (1,)), ((), ())), preferred_element_type=jnp.float32)


def dot_n(a, b):
    return lax.dot_general(a, b, (((1,), (0,)), ((), ())), preferred_element_type=jnp.float32)


def lead_kernel(keys_ref, values_ref, k_out, v_out, sems):
    copies = [
        pltpu.make_async_copy(src.at[pl.ds(0, dst.shape[0])], dst, sems.at[i])
        for i, (src, dst) in enumerate(((keys_ref, k_out), (values_ref, v_out)))
    ]
    for copy in copies:
        copy.start()
    for copy in copies:
        copy.wait()


def in_hbm(x):
    return pltpu.with_memory_space_constraint(x, pltpu.HBM)


HBM = pl.BlockSpec(memory_space=pltpu.HBM)
VMEM = pl.BlockSpec(memory_space=pltpu.VMEM)
SMEM = pl.BlockSpec(memory_space=pltpu.SMEM)


def lead_pages(keys, values):
    out = jax.ShapeDtypeStruct((HOT_CAP, *keys.shape[1:]), keys.dtype)
    return pl.pallas_call(
        lead_kernel,
        out_shape=(out, out),
        in_specs=[HBM, HBM],
        out_specs=(VMEM, VMEM),
        scratch_shapes=[pltpu.SemaphoreType.DMA((2,))],
        compiler_params=pltpu.CompilerParams(vmem_limit_bytes=4 * MIB),
        name="lead_pages",
    )(in_hbm(keys), in_hbm(values))


def own_kernel(
    seqs, ups, heads, group, kv_heads,
    pages_ref, lengths_ref, q_ref, first_k, last_k, first_v, v_hbm,
    num_ref, tot_ref, last_v, tail_sem,
):
    page_len, head_dim = first_v.shape[2:]
    early, late = first_k.shape[0], last_k.shape[0]

    def tail(act):
        def one(i, carry):
            act(pltpu.make_async_copy(v_hbm.at[pages_ref[early + i]], last_v.at[i], tail_sem.at[i]))
            return carry

        lax.fori_loop(0, late, one, 0)

    tail(lambda copy: copy.start())
    width = kv_heads * page_len
    column = lax.broadcasted_iota(jnp.int32, (heads, width), 1)
    row = lax.broadcasted_iota(jnp.int32, (heads, width), 0)
    mine = (column // page_len) == (row // group)
    token = jnp.where(mine, column % page_len, ups * page_len)
    ones = jnp.ones((width, head_dim), jnp.bfloat16)
    done = 0
    for kbuf, vbuf in ((first_k, first_v), (last_k, last_v)):
        if kbuf is last_k:
            tail(lambda copy: copy.wait())
        part = kbuf.shape[0] // ups
        unroll = math.gcd(part, 16)

        def block(b, carry, first=done, unroll=unroll, kbuf=kbuf, vbuf=vbuf):
            for j in range(unroll):
                at = b * unroll + j
                s = first + at
                q = q_ref[pl.ds(pl.multiple_of(s * heads, heads), heads), :]
                total = jnp.zeros((heads, 2 * head_dim), jnp.float32)
                for u in range(ups):
                    k = kbuf[at * ups + u].reshape(width, head_dim)
                    v = vbuf[at * ups + u].reshape(width, head_dim)
                    allowed = token < lengths_ref[s] - u * page_len
                    weight = jnp.where(allowed, weights_of(dot_t(q, k)), 0.0).astype(jnp.bfloat16)
                    total = total + dot_n(weight, jnp.concatenate([v, ones], axis=1))
                num_ref[pl.ds(s, heads, stride=seqs), :] = total[:, :head_dim]
                tot_ref[pl.ds(s, heads, stride=seqs), :] = total[:, head_dim:]
            return carry

        lax.fori_loop(0, part // unroll, block, 0)
        done += part


def own_terms(q, pages, own_k, first_v, values, lengths):
    seqs, _, head_dim = q.shape
    _, kv_heads, page_len, _ = first_v.shape
    count, late = pages.shape[0], own_k[1].shape[0]
    group = q.shape[1] // kv_heads
    heads = -(-q.shape[1] // 8) * 8
    q = jnp.pad(q, ((0, 0), (0, heads - q.shape[1]), (0, 0))).reshape(seqs * heads, head_dim)
    out = jax.ShapeDtypeStruct((heads * seqs, head_dim), jnp.float32)
    return pl.pallas_call(
        functools.partial(own_kernel, seqs, count // seqs, heads, group, kv_heads),
        out_shape=(out, out),
        in_specs=[SMEM, SMEM] + [VMEM] * 4 + [HBM],
        out_specs=(VMEM, VMEM),
        scratch_shapes=[
            pltpu.VMEM((late, kv_heads, page_len, head_dim), values.dtype),
            pltpu.SemaphoreType.DMA((late,)),
        ],
        compiler_params=pltpu.CompilerParams(vmem_limit_bytes=8 * MIB),
        name="own_pages",
    )(pages, lengths, q, *own_k, first_v, in_hbm(values))


def shared_places(me, cap, page_count, hot_ref, lanes):
    shape = (2 * cap, hot_ref.shape[1])
    slot = lax.broadcasted_iota(jnp.int32, shape, 0)
    lane = lax.broadcasted_iota(jnp.int32, shape, 1).astype(jnp.float32)
    first = jnp.where(slot < cap, me * page_count, (me ^ 1) * page_count - cap)
    matches = jnp.broadcast_to(hot_ref[...], shape) == first + slot
    place = jnp.min(jnp.where(matches, lane, 1e9), axis=1, keepdims=True)
    return jnp.broadcast_to(place, (2 * cap, lanes))


def used_column(origin, seqs, used_ref, lanes):
    span = used_ref.shape[1]
    row = used_ref[pl.ds(origin * seqs // span, 1), :].astype(jnp.float32)
    shape = (seqs, span)
    lane = lax.broadcasted_iota(jnp.int32, shape, 1)
    sequence = lax.broadcasted_iota(jnp.int32, shape, 0) + origin * seqs % span
    picked = jnp.where(lane == sequence, jnp.broadcast_to(row, shape), 0.0)
    return jnp.broadcast_to(jnp.sum(picked, axis=1, keepdims=True), (seqs, lanes))


def hot_kernel(sources, halves, seqs, heads, kv_heads, fetches, page_count, hot_ref, used_ref, *refs):
    pages_ref, *refs = refs
    jobs = len(fetches)
    caches, refs = refs[:jobs], refs[jobs:]
    refs, fetched, (staged, places), sems = (
        refs[: -2 * jobs - 2], refs[-2 * jobs - 2 : -jobs - 2], refs[-jobs - 2 : -jobs], refs[-jobs:]
    )

    def each(act):
        for n, (first, last) in enumerate(fetches):

            def one(i, carry, n=n, first=first):
                src = caches[n].at[pages_ref[first + i]]
                act(pltpu.make_async_copy(src, fetched[n].at[i], sems[n].at[i]))
                return carry

            lax.fori_loop(0, last - first, one, 0)

    each(lambda copy: copy.start())
    count = len(sources)
    queries, refs = refs[:count], refs[count:]
    kv = [(refs[2 * i], refs[2 * i + 1]) for i in range(len(halves))]
    outs = list(refs[2 * len(halves) :])
    group = heads // kv_heads
    cap, _, page_len, head_dim = kv[0][0].shape
    lane = lax.broadcasted_iota(jnp.int32, (8, head_dim), 1)
    for r in range(count):
        staged[r] = queries[r][...].astype(jnp.float32)
    me = lax.axis_index("pages")
    places[...] = shared_places(me, cap, page_count, hot_ref, head_dim)
    used_rows = [used_column(shift(me), seqs, used_ref, head_dim) for shift, _, _ in sources]
    step = 2
    ones = jnp.ones((step * page_len, head_dim), jnp.bfloat16)
    dests = []
    for _, _, packed in sources:
        dests.append(outs.pop(0) if packed else (outs.pop(0), outs.pop(0)))
    totals = [jnp.zeros((8, head_dim), jnp.float32) for _ in range(count)]
    for h in range(kv_heads):
        rows = [
            [
                staged[r, pl.ds(h * group + g, seqs, stride=heads), :].astype(jnp.bfloat16)
                for g in range(group)
            ]
            for r in range(count)
        ]
        acc = [jnp.zeros((group * seqs, 2 * head_dim), jnp.float32) for _ in range(count)]
        for half, (k_ref, v_ref) in zip(halves, kv):
            active = [r for r in range(count) if half in sources[r][1]]
            q = jnp.concatenate([row for r in active for row in rows[r]], axis=0)
            for c in range(0, cap, step):
                k = k_ref[c : c + step, h].reshape(step * page_len, head_dim)
                v = v_ref[c : c + step, h].reshape(step * page_len, head_dim)
                weight = weights_of(dot_t(q, k))
                parts = []
                for p in range(step):
                    slot = half * cap + c + p
                    place = jnp.broadcast_to(places[slot : slot + 1, :], (seqs, page_len))
                    columns = slice(p * page_len, (p + 1) * page_len)
                    part = []
                    for n, r in enumerate(active):
                        mask = used_rows[r] > place
                        for i in range(n * group, (n + 1) * group):
                            part.append(jnp.where(mask, weight[i * seqs : (i + 1) * seqs, columns], 0.0))
                    parts.append(jnp.concatenate(part, axis=0).astype(jnp.bfloat16))
                res = dot_n(jnp.concatenate(parts, axis=1), jnp.concatenate([v, ones], axis=1))
                for n, r in enumerate(active):
                    acc[r] = acc[r] + res[n * group * seqs : (n + 1) * group * seqs]
        for r, (_, _, packed) in enumerate(sources):
            for g in range(group):
                head = h * group + g
                num = acc[r][g * seqs : (g + 1) * seqs, :head_dim]
                tot = acc[r][g * seqs : (g + 1) * seqs, head_dim:]
                if packed:
                    rest = tot - tot.astype(jnp.bfloat16).astype(jnp.float32)
                    dests[r][head * seqs : (head + 1) * seqs, :] = num.astype(jnp.bfloat16)
                    for j in range(seqs // 8):
                        at, fold = 2 * heads * j + head, slice(8 * j, 8 * j + 8)
                        low = jnp.where(lane == at + heads, rest[fold], totals[r])
                        totals[r] = jnp.where(lane == at, tot[fold], low)
                else:
                    dests[r][0][head * seqs : (head + 1) * seqs, :] = num
                    dests[r][1][head * seqs : (head + 1) * seqs, :] = tot
    for r, (_, _, packed) in enumerate(sources):
        if packed:
            padded = jnp.concatenate([totals[r], jnp.zeros_like(totals[r])], axis=0)
            dests[r][heads * seqs :, :] = padded.astype(jnp.bfloat16)
    each(lambda copy: copy.wait())


def hot_terms(queries, sources, halves, kv, page_count, tables, pages, fetch):
    _, kv_heads, page_len, head_dim = kv[0].shape
    seqs, heads = queries[0].shape[:2]
    shapes = []
    for _, _, packed in sources:
        if packed:
            shapes.append(((heads * seqs + 16, head_dim), jnp.bfloat16))
        else:
            shapes += [((heads * seqs, head_dim), jnp.float32)] * 2
    counts = [last - first for _, first, last in fetch]
    shapes += [((n, kv_heads, page_len, head_dim), kv[0].dtype) for n in counts]
    fetches = tuple((first, last) for _, first, last in fetch)
    flat = [q.reshape(seqs * heads, head_dim) for q in queries]
    operands = [*tables, pages, *(in_hbm(f[0]) for f in fetch), *flat, *kv]
    return pl.pallas_call(
        functools.partial(
            hot_kernel, sources, halves, seqs, heads, kv_heads, fetches, page_count
        ),
        out_shape=[jax.ShapeDtypeStruct(*s) for s in shapes],
        in_specs=[VMEM, VMEM, SMEM] + [HBM] * len(fetch) + [VMEM] * (len(flat) + len(kv)),
        out_specs=[VMEM] * len(shapes),
        scratch_shapes=[
            pltpu.VMEM((len(sources), seqs * heads, head_dim), jnp.float32),
            pltpu.VMEM((2 * HOT_CAP, head_dim), jnp.float32),
            *(pltpu.SemaphoreType.DMA((n,)) for n in counts),
        ],
        compiler_params=pltpu.CompilerParams(vmem_limit_bytes=12 * MIB),
        name="hot_pages",
    )(*operands)


def row_owner(i, k, ways):
    return i ^ k if ways & (ways - 1) == 0 else lax.rem(i + k, ways)


def row_order(ways):
    return [2, 1, 3] if ways == 4 else list(range(ways - 1, 0, -1))


def project_kernel(received, seqs, heads, ways, *refs):
    blocks = refs[:received]
    nums, tots = refs[received : received + 3], refs[received + 3 : received + 6]
    w_ref, outs, spread = refs[received + 6], refs[received + 7 : received + 7 + ways], refs[-1]
    head_dim = nums[0].shape[1]
    rows = seqs // ways
    far = jnp.zeros((16, head_dim), jnp.float32)
    for b in blocks:
        far = far + b[heads * seqs :, :].astype(jnp.float32)
    for h in range(heads):
        part = pl.ds(h * seqs, seqs)
        num = nums[0][part, :] + nums[1][part, :] + nums[2][part, :]
        tot = tots[0][part, :] + tots[1][part, :] + tots[2][part, :]
        for b in blocks:
            num = num + b[part, :].astype(jnp.float32)
        if blocks:
            folds = []
            for at in range(h, 2 * heads * (seqs // 8), 2 * heads):
                fold = far[:8, at : at + 1] + far[:8, at + heads : at + heads + 1]
                folds.append(jnp.broadcast_to(fold, (8, head_dim)))
            tot = tot + jnp.concatenate(folds, axis=0)
        spread[:, h * head_dim : (h + 1) * head_dim] = num / tot
    turned = []
    for k in range(ways):
        target = row_owner(lax.axis_index("heads"), k, ways)
        turned.append(spread[pl.ds(pl.multiple_of(target * rows, rows), rows), :])
    att = jnp.concatenate(turned, axis=0).astype(jnp.bfloat16)
    model = w_ref.shape[1]
    tile = math.gcd(model, 768)
    for n in range(0, model, tile):
        res = dot_n(att, w_ref[:, n : n + tile])
        for k in range(ways):
            outs[k][:, n : n + tile] = res[k * rows : (k + 1) * rows].astype(outs[k].dtype)


def project(blocks, near, rest, own, o_weight, ways):
    head_dim = own[0].shape[1]
    width, model = o_weight.shape
    heads = width // head_dim
    seqs = near[0].shape[0] // heads
    rows = seqs // ways
    kinds = [jnp.float32] + [jnp.bfloat16] * (ways - 1)
    return pl.pallas_call(
        functools.partial(project_kernel, len(blocks), seqs, heads, ways),
        out_shape=[jax.ShapeDtypeStruct((rows, model), kind) for kind in kinds],
        in_specs=[VMEM] * (len(blocks) + 7),
        out_specs=[VMEM] * ways,
        scratch_shapes=[pltpu.VMEM((seqs, width), jnp.float32)],
        compiler_params=pltpu.CompilerParams(vmem_limit_bytes=8 * MIB),
        name="project",
    )(*blocks, near[0], rest[0], own[0], near[1], rest[1], own[1], o_weight)


def norm_kernel(*refs):
    parts, (residual, gain, out) = refs[:-3], refs[-3:]
    projected = parts[0][...]
    for p in parts[1:]:
        projected = projected + p[...].astype(jnp.float32)
    mean_sq = jnp.mean(projected * projected, axis=1, keepdims=True)
    normed = projected / jnp.sqrt(mean_sq + epsilon) * gain[...]
    out[...] = (residual[...].astype(jnp.float32) + normed).astype(jnp.bfloat16)


def finish(parts, residual, norm_gain):
    return pl.pallas_call(
        norm_kernel,
        out_shape=jax.ShapeDtypeStruct(residual.shape, residual.dtype),
        compiler_params=pltpu.CompilerParams(vmem_limit_bytes=8 * MIB),
        name="finish",
    )(*parts, residual, norm_gain.reshape(1, -1))


def layer(
    chips, ways, queries, keys, values, hot_pages, hot_used, user_pages, lengths, o_weight, residual, norm_gain
):
    page_count = keys.shape[0]
    devices = 2 * chips
    swap = [(i, i ^ 1) for i in range(devices)]
    power = chips & (chips - 1) == 0

    def there(i, k):
        return i ^ (2 * k) if power else (i + 2 * k) % devices

    pages = user_pages.reshape(-1)
    out_perm = [[(i, there(i, k)) for i in range(devices)] for k in range(chips)]
    back_perm = [[(j, i) for i, j in perm] for perm in out_perm]
    far_q = []
    for k in range(1, chips):
        far_q.append(lax.ppermute(queries, "pages", out_perm[k]))
    own_kv = lead_pages(keys, values)
    partner_kv = tuple(lax.ppermute(x, "pages", swap) for x in own_kv)

    def shift(k):
        if power:
            return lambda i: i ^ (2 * k)
        return lambda i: lax.rem(i + devices - 2 * k, devices)

    tables = (hot_pages.reshape(1, -1), hot_used.reshape(-1, 128))
    count = pages.shape[0]
    early = count // 4 * 3 // user_pages.shape[1] * user_pages.shape[1]
    *near, first_k = hot_terms(
        [queries], [(shift(0), (0,), False)], (0,), own_kv, page_count, tables, pages,
        [(keys, 0, early)],
    )
    near, far_q, partner_kv = lax.optimization_barrier((near, far_q, partner_kv))
    sources = [(shift(k), (0, 1), True) for k in range(1, chips)] + [(shift(0), (1,), False)]
    *sent, rest_num, rest_tot, last_k, first_v = hot_terms(
        [*far_q, queries], sources, (0, 1), (*own_kv, *partner_kv), page_count, tables, pages,
        [(keys, early, count), (values, 0, early)],
    )
    blocks = []
    for k, b in zip(range(1, chips), sent):
        blocks.append(lax.ppermute(b, "pages", back_perm[k]))
    queries, rest_num = lax.optimization_barrier((queries, rest_num))
    own = own_terms(
        queries, pages, (first_k, last_k), first_v, values, lengths
    )
    parts = project(blocks, near, (rest_num, rest_tot), own, o_weight, ways)
    arrived = [parts[0]]
    for k in row_order(ways):
        pairs = [(i, i ^ k if ways & (ways - 1) == 0 else (i + k) % ways) for i in range(ways)]
        arrived.append(lax.ppermute(parts[k], "heads", pairs))
    return finish(arrived, residual, norm_gain)


def solution(mesh):
    in_specs = (
        P("pages", "heads", None),
        P("pages", "heads", None, None),
        P("pages", "heads", None, None),
        P(),
        P(),
        P("pages", None),
        P("pages"),
        P("heads", None),
        P(("pages", "heads"), None),
        P(),
    )
    out_specs = P(("pages", "heads"), None)
    chips = mesh.shape["pages"] // 2
    body = functools.partial(layer, chips, mesh.shape["heads"])
    return jax.shard_map(body, mesh=mesh, in_specs=in_specs, out_specs=out_specs, check_vma=False)
```
